32 devices in a mesh: dp: 1, tp: 32 (over x, y, z, core).
Axes of the slice: x: 2, y: 2, z: 4, core: 2. Of those that a mesh axis runs over, the one named last changes fastest.
Arguments:
- x: bfloat16 [2048, 5120], P('dp')
- dy: bfloat16 [2048, 5120], P('dp')
- gate: bfloat16 [2048, 12288], P('dp', 'tp')
- up: bfloat16 [2048, 12288], P('dp', 'tp')
- w_gate: bfloat16 [5120, 12288], P(None, 'tp')
- w_up: bfloat16 [5120, 12288], P(None, 'tp')
- w_down: bfloat16 [12288, 5120], P('tp')
Outputs:
- output 1: bfloat16 [2048, 5120], P('dp')
- output 2: bfloat16 [5120, 12288], P('dp', 'tp')
- output 3: bfloat16 [5120, 12288], P('dp', 'tp')
- output 4: bfloat16 [12288, 5120], P(('dp', 'tp'))
All inputs are finite; a program needn't handle non-finite values.
Results may differ from the reference program's by a relative error of at most 0.012.
Values are sent between devices in bfloat16 or wider.
A program may use at most 2 GiB of HBM per device.

```python
import jax
import jax.numpy as jnp

ROWS = 2048
D = 5120
FF = 12288


def act(gate, up):
    return jax.nn.silu(gate) * up


def setup_inputs(seed: int = 0, part: int = 0) -> dict:
    kx, ky, ka, kb, kg, ku, kd = jax.random.split(jax.random.key(seed), 7)
    kx, ky, ka, kb = (jax.random.fold_in(k, part) for k in (kx, ky, ka, kb))
    drawn = {
        "x": jax.random.normal(kx, (ROWS, D), jnp.float32),
        "dy": jax.random.normal(ky, (ROWS, D), jnp.float32),
        "gate": jax.random.normal(ka, (ROWS, FF), jnp.float32),
        "up": jax.random.normal(kb, (ROWS, FF), jnp.float32),
        "w_gate": jax.random.normal(kg, (D, FF), jnp.float32) * D**-0.5,
        "w_up": jax.random.normal(ku, (D, FF), jnp.float32) * D**-0.5,
        "w_down": jax.random.normal(kd, (FF, D), jnp.float32) * FF**-0.5,
    }
    return {k: v.astype(jnp.bfloat16) for k, v in drawn.items()}


def reference(x, dy, gate, up, w_gate, w_up, w_down):
    hidden, back = jax.vjp(act, gate.astype(jnp.float32), up.astype(jnp.float32))
    d_hidden = jnp.dot(dy, w_down.T, preferred_element_type=jnp.float32)
    d_gate, d_up = (g.astype(jnp.bfloat16) for g in back(d_hidden))
    dx = jnp.dot(d_gate, w_gate.T, preferred_element_type=jnp.float32) + jnp.dot(d_up, w_up.T, preferred_element_type=jnp.float32)
    dw_gate = jnp.dot(x.T, d_gate, preferred_element_type=jnp.float32)
    dw_up = jnp.dot(x.T, d_up, preferred_element_type=jnp.float32)
    dw_down = jnp.dot(hidden.astype(jnp.bfloat16).T, dy, preferred_element_type=jnp.float32)
    return tuple(g.astype(jnp.bfloat16) for g in (dx, dw_gate, dw_up, dw_down))
```

```python
import jax
import jax.numpy as jnp
from jax import lax
from jax.experimental import pallas as pl
from jax.experimental.pallas import tpu as pltpu
from jax.sharding import PartitionSpec as P

MESH = pl.DeviceIdType.MESH
R = 1024


class Comm:
    def __init__(self, G, D, cw, pA=320, KS=None):
        self.G, self.D, self.cw = G, D, cw
        self.K = KS or 3 * D
        self.a = pA; self.h = pA // 2; self.q = pA // 4
        self.e = R - 2 * pA; self.b = self.e // 4
        assert self.q % 16 == 0 and self.b % 16 == 0
        self.NS = 10
        self.rx = dict(A0=self.h, B0=self.h, A1=self.q, B1=self.q, A2=self.q, B2=self.q, A3=self.q, B3=self.q,
                       E0=3*self.b, E1=2*self.b, E2=self.b, EX=self.b, EY=self.b)
        off = 0; self.off = {}
        for k, v in self.rx.items():
            self.off[k] = off; off += v
        self.rxrows = off
        self.kinds = {}
        for i in range(8):
            self.kinds['A%d' % i] = len(self.kinds); self.kinds['B%d' % i] = len(self.kinds)
        for i in range(9):
            self.kinds['E%d' % i] = len(self.kinds)
        self.kinds['D'] = len(self.kinds); self.kinds['L'] = len(self.kinds)

    def scratch(self):
        n = len(self.kinds)
        return [pltpu.VMEM((self.G, R, self.cw), jnp.bfloat16),
                pltpu.VMEM((self.K, self.rxrows, self.cw), jnp.bfloat16),
                pltpu.SemaphoreType.DMA((n, self.K)), pltpu.SemaphoreType.DMA((n, self.K)), pltpu.SemaphoreType.REGULAR]

    def bind(self, work, rxb, ssem, rsem, credit, out):
        self.work, self.rxb, self.ssem, self.rsem, self.credit, self.out = work, rxb, ssem, rsem, credit, out
        me = lax.axis_index("tp")
        core = me % 2; z = (me // 2) % 4; y = (me // 8) % 2; x = me // 16
        idx = lambda x, y, z, c: ((x * 2 + y) * 4 + z) * 2 + c
        self.core, self.z, self.y, self.x = core, z, y, x
        side = z // 2; self.side = side
        self.outer = jnp.logical_or(z == 0, z == 3); self.inner = jnp.logical_not(self.outer)
        zi = 1 + side
        zo = 3 * side
        self.px = idx(1 - x, y, z, core); self.py = idx(x, 1 - y, z, core)
        self.pc = idx(x, y, z, 1 - core)
        self.pin = idx(x, y, zi, core)
        self.pout = idx(x, y, zo, core)
        self.pacr = idx(x, y, 2 - side, core)
        m = lambda v: pl.multiple_of(v, 16)
        a, h, q, b = self.a, self.h, self.q, self.b
        e0 = 2 * a
        self.Ak = m(x * h); self.As = m((1 - x) * h)
        self.Aq = m(x * h + y * q); self.Aqs = m(x * h + (1 - y) * q)
        self.Bk = m(a + y * h); self.Bs = m(a + (1 - y) * h)
        self.Bq = m(a + y * h + x * q); self.Bqs = m(a + y * h + (1 - x) * q)
        self.Eex = m(e0 + (1 - side) * b); self.Efar = m(e0 + (1 - side) * 2 * b); self.Enear = m(e0 + side * 2 * b)
        self.Eown = m(e0 + z * b); self.Eout = m(e0 + zo * b)

    def barrier(self):
        bar = pltpu.get_barrier_semaphore()
        def sig(d): pl.semaphore_signal(bar, inc=1, device_id={"tp": d}, device_id_type=MESH)
        sig(self.px); sig(self.py); sig(self.pc)
        @pl.when(self.outer)
        def _(): sig(self.pin); pl.semaphore_wait(bar, 4)
        @pl.when(self.inner)
        def _(): sig(self.pout); sig(self.pacr); pl.semaphore_wait(bar, 5)

    def cp(self, kind, c, start, rows, dst_kind, dev):
        k = self.kinds[kind]; sl = c % self.K
        src = self.work.at[c, pl.ds(start, rows), :]
        if dst_kind is None: dst = src
        else: dst = self.rxb.at[sl, pl.ds(self.off[dst_kind], rows), :]
        return pltpu.make_async_remote_copy(src_ref=src, dst_ref=dst, send_sem=self.ssem.at[k, sl], recv_sem=self.rsem.at[k, sl],
                                            device_id={"tp": dev}, device_id_type=MESH)

    def add(self, c, start, rows, rxk, roff=0):
        sl = c % self.K
        w = self.work.at[c, pl.ds(start, rows), :]
        v = w[...].astype(jnp.float32) + self.rxb[sl, pl.ds(self.off[rxk] + roff, rows), :].astype(jnp.float32)
        w[...] = v.astype(jnp.bfloat16)

    def stage(self, s, c):
        q, h, b = self.q, self.h, self.b
        C = self.cp
        A = [lambda: C('A0', c, self.As, h, 'A0', self.px), lambda: C('A1', c, self.Aqs, q, 'A1', self.py),
             lambda: C('A2', c, self.Aq, q, 'A2', self.pin), lambda: C('A3', c, self.Aq, q, 'A3', self.pacr),
             lambda: C('A4', c, self.Aq, q, None, self.pout), lambda: C('A5', c, self.Aq, q, None, self.py),
             lambda: C('A6', c, self.Ak, h, None, self.px)]
        B = [lambda: C('B0', c, self.Bs, h, 'B0', self.py), lambda: C('B1', c, self.Bqs, q, 'B1', self.px),
             lambda: C('B2', c, self.Bq, q, 'B2', self.pin), lambda: C('B3', c, self.Bq, q, 'B3', self.pacr),
             lambda: C('B4', c, self.Bq, q, None, self.pout), lambda: C('B5', c, self.Bq, q, None, self.px),
             lambda: C('B6', c, self.Bk, h, None, self.py)]
        E = [lambda: C('E0', c, self.Eex, 3*b, 'E0', self.pin), lambda: C('E1', c, self.Efar, 2*b, 'E1', self.pacr),
             lambda: C('E2', c, self.Eout, b, 'E2', self.pout), lambda: C('E3', c, self.Eown, b, 'EX', self.px),
             lambda: C('E4', c, self.Eown, b, 'EY', self.py), lambda: C('E5', c, self.Eown, b, None, self.pin),
             lambda: C('E6', c, self.Enear, 2*b, None, self.pacr), lambda: C('E7', c, self.Eex, 3*b, None, self.pout)]
        ws = lambda d: d().wait_send()
        wr = lambda d: d().wait_recv()
        st = lambda d: d().start()
        outer = lambda f: pl.when(self.outer)(f)
        inner = lambda f: pl.when(self.inner)(f)
        if s == 0:
            st(A[0]); st(B[0])
            @outer
            def _(): st(E[0])
        elif s == 1:
            @inner
            def _(): wr(E[0]); self.add(c, self.Eex, 3*b, 'E0'); st(E[1])
            @outer
            def _(): ws(E[0])
            A[0]().wait(); self.add(c, self.Ak, h, 'A0'); st(A[1])
            B[0]().wait(); self.add(c, self.Bk, h, 'B0'); st(B[1])
        elif s == 2:
            @inner
            def _(): E[1]().wait(); self.add(c, self.Enear, 2*b, 'E1'); st(E[2])
            A[1]().wait(); self.add(c, self.Aq, q, 'A1')
            @outer
            def _(): st(A[2])
            B[1]().wait(); self.add(c, self.Bq, q, 'B1')
            @outer
            def _(): st(B[2])
        elif s == 3:
            @inner
            def _():
                ws(E[2])
                wr(A[2]); self.add(c, self.Aq, q, 'A2'); st(A[3])
                wr(B[2]); self.add(c, self.Bq, q, 'B2'); st(B[3])
            @outer
            def _(): wr(E[2]); self.add(c, self.Eown, b, 'E2'); ws(A[2]); ws(B[2]); pl.semaphore_signal(self.credit, inc=1, device_id={"tp": self.pin}, device_id_type=MESH)
            st(E[3])
        elif s == 4:
            @inner
            def _():
                pl.semaphore_wait(self.credit, 1)
                A[3]().wait(); self.add(c, self.Aq, q, 'A3'); st(A[4])
                B[3]().wait(); self.add(c, self.Bq, q, 'B3'); st(B[4])
            E[3]().wait(); self.add(c, self.Eown, b, 'EX'); st(E[4])
        elif s == 5:
            E[4]().wait(); self.add(c, self.Eown, b, 'EY')
            @outer
            def _(): wr(A[4]); wr(B[4]); st(E[5])
            @inner
            def _(): ws(A[4])
            st(A[5])
            @inner
            def _(): ws(B[4])
            st(B[5])
        elif s == 6:
            @inner
            def _(): wr(E[5]); st(E[6])
            @outer
            def _(): ws(E[5])
            A[5]().wait(); st(A[6])
            B[5]().wait(); st(B[6])
        elif s == 7:
            @inner
            def _(): E[6]().wait(); st(E[7])
            A[6]().wait(); B[6]().wait()
        elif s == 8:
            @inner
            def _(): ws(E[7])
            @outer
            def _(): wr(E[7])
            d, l = self.final(c); d.start(); l.start()
        elif s == 9:
            d, l = self.final(c); d.wait(); l.wait()

    def final(self, c):
        sl = c % self.K
        dst = self.out.at[pl.ds(pl.multiple_of(self.core * R, R), R), pl.ds(pl.multiple_of(c * self.cw, self.cw), self.cw)]
        src = self.work.at[c]
        k = self.kinds['D']; k2 = self.kinds['L']
        d = pltpu.make_async_remote_copy(src_ref=src, dst_ref=dst, send_sem=self.ssem.at[k, sl], recv_sem=self.rsem.at[k, sl],
                                         device_id={"tp": self.pc}, device_id_type=MESH)
        l = pltpu.make_async_copy(src, dst, self.ssem.at[k2, sl])
        return d, l

    def tick(self, t):
        for s in reversed(range(self.NS)):
            c = t - self.D * s
            @pl.when(jnp.logical_and(c >= 0, c < self.G))
            def _(s=s, c=c): self.stage(s, c)
    @property
    def nticks(self): return self.G + self.D * (self.NS - 1)


T, D, F = 2048, 5120, 384
G, SPACING, CW = 40, 2, 128
RB = 256
NB = T // RB
UW = 256
NU = D // UW
PIECES = 5
UNIT0 = 5


def nt(a, b):
    return lax.dot_general(a, b, (((1,), (1,)), ((), ())), preferred_element_type=jnp.float32)


def nn(a, b):
    return jnp.dot(a, b, preferred_element_type=jnp.float32)


def kernel(comm, x, dy, gate, up, w_gate, w_up, w_down, dx, dwg, dwu, dwd,
           work, rxb, ssem, rsem, credit, wown, wfar, dall, dfar, dall_t, hid_t,
           own_sem, far_s, far_r, df_s, df_r):
    comm.bind(work, rxb, ssem, rsem, credit, dx)
    mine = pl.multiple_of(comm.core * R, R)
    theirs = pl.multiple_of((1 - comm.core) * R, R)
    own = [pltpu.make_async_copy(w, wown.at[:, pl.ds(i * F, F)], own_sem.at[i]) for i, w in enumerate((w_gate, w_up))]
    PR = D // PIECES

    def far(i, p):
        rows = pl.ds(pl.multiple_of(p * PR, PR), PR)
        return pltpu.make_async_remote_copy(
            src_ref=(w_gate, w_up)[i].at[rows], dst_ref=wfar.at[rows, pl.ds(i * F, F)], send_sem=far_s.at[i, p],
            recv_sem=far_r.at[i, p], device_id={"tp": comm.pc}, device_id_type=MESH)

    def dsend(b):
        return pltpu.make_async_remote_copy(
            src_ref=dall.at[pl.ds(pl.multiple_of(theirs + b * RB, RB), RB)],
            dst_ref=dfar.at[pl.ds(pl.multiple_of(b * RB, RB), RB)], send_sem=df_s.at[b], recv_sem=df_r.at[b],
            device_id={"tp": comm.pc}, device_id_type=MESH)

    def hidden_part(wd, dyb, gb, ub, sem):
        pre = [pltpu.make_async_copy(s, d, sem.at[2 + i]) for i, (s, d) in enumerate(((w_down, wd), (gate, gb), (up, ub)))]

        def row0(b):
            return pl.multiple_of(lax.rem(theirs + b * RB, T), RB)

        def load(b):
            return pltpu.make_async_copy(dy.at[pl.ds(row0(b), RB)], dyb.at[lax.rem(b, 2)], sem.at[lax.rem(b, 2)])

        load(0).start()
        for c in pre:
            c.start()
        comm.barrier()
        for p in range(PIECES):
            for i in range(2):
                far(i, p).start()
        for c in own:
            c.start()
        for c in pre:
            c.wait()

        def step(b, _):
            @pl.when(b + 1 < NB)
            def _():
                load(b + 1).start()
            load(b).wait()
            rows = pl.ds(row0(b), RB)
            dh = nt(dyb[lax.rem(b, 2)], wd[...])
            g, u = gb[rows, :].astype(jnp.float32), ub[rows, :].astype(jnp.float32)
            sig = jax.nn.sigmoid(g)
            silu = g * sig
            d_up = (dh * silu).astype(jnp.bfloat16)
            d_gate = (dh * u * (sig + silu * (1.0 - sig))).astype(jnp.bfloat16)
            hid = (silu * u).astype(jnp.bfloat16)
            dall[rows, 0:F] = d_gate
            dall[rows, F:2 * F] = d_up
            dall_t[0:F, rows] = d_gate.T
            dall_t[F:2 * F, rows] = d_up.T
            hid_t[:, rows] = hid.T

            @pl.when(b < NB // 2)
            def _():
                dsend(b).start()
            return 0

        lax.fori_loop(0, NB, step, 0)

    pl.run_scoped(hidden_part, pltpu.VMEM((F, D), jnp.bfloat16), pltpu.VMEM((2, RB, D), jnp.bfloat16),
                  pltpu.VMEM((T, F), jnp.bfloat16), pltpu.VMEM((T, F), jnp.bfloat16), pltpu.SemaphoreType.DMA((5,)))

    def terms(pair):
        per = PR // (2 * CW)

        @pl.when(lax.rem(pair, per) == 0)
        def _():
            for i in range(2):
                far(i, pair // per).wait()
        rows = pl.ds(pl.multiple_of(pair * 2 * CW, 2 * CW), 2 * CW)
        for half in range(2):
            r = pl.ds(half * R // 2, R // 2)
            t = nt(dall[pl.ds(pl.multiple_of(mine + half * R // 2, R // 2), R // 2), :], wown[rows, :]) + nt(dfar[r, :], wfar[rows, :])
            t = t.astype(jnp.bfloat16)
            work[2 * pair, r, :] = t[:, :CW]
            work[2 * pair + 1, r, :] = t[:, CW:]

    def main_part(xb, dyb, og, od, lsem, osem):
        def loads(u):
            s = lax.rem(u, 2)
            cols = pl.ds(pl.multiple_of(u * UW, UW), UW)
            return [pltpu.make_async_copy(x.at[:, cols], xb.at[s], lsem.at[0, s]),
                    pltpu.make_async_copy(dy.at[:, cols], dyb.at[s], lsem.at[1, s])]

        def stores(u):
            s = lax.rem(u, 2)
            cols = pl.ds(pl.multiple_of(u * UW, UW), UW)
            return [pltpu.make_async_copy(og.at[s, 0], dwg.at[cols], osem.at[0, s]),
                    pltpu.make_async_copy(og.at[s, 1], dwu.at[cols], osem.at[1, s]),
                    pltpu.make_async_copy(od.at[s], dwd.at[:, cols], osem.at[2, s])]

        for c in loads(0):
            c.start()
        for b in range(NB // 2):
            dsend(b).wait()
        for c in own:
            c.wait()
        terms(0)

        def unit(u):
            s = lax.rem(u, 2)

            @pl.when(u + 1 < NU)
            def _():
                for c in loads(u + 1):
                    c.start()
            for c in loads(u):
                c.wait()

            @pl.when(u >= 2)
            def _():
                for c in stores(u - 2):
                    c.wait()
            for i in range(2):
                og[s, i] = nn(dall_t[pl.ds(i * F, F), :], xb[s]).T.astype(jnp.bfloat16)
            od[s] = nn(hid_t[...], dyb[s]).astype(jnp.bfloat16)
            for c in stores(u):
                c.start()

        def tick(t, _):
            comm.tick(t)
            pair = t // 2 + 1

            @pl.when(jnp.logical_and(lax.rem(t, 2) == 0, pair < G // 2))
            def _():
                terms(pair)
            u = (t - UNIT0) // 2

            @pl.when(jnp.logical_and(jnp.logical_and(t >= UNIT0, lax.rem(t - UNIT0, 2) == 0), u < NU))
            def _():
                unit(u)
            return 0

        lax.fori_loop(0, comm.nticks, tick, 0)
        for u in (NU - 2, NU - 1):
            for c in stores(u):
                c.wait()

    pl.run_scoped(main_part, pltpu.VMEM((2, T, UW), jnp.bfloat16), pltpu.VMEM((2, T, UW), jnp.bfloat16),
                  pltpu.VMEM((2, 2, UW, F), jnp.bfloat16), pltpu.VMEM((2, F, UW), jnp.bfloat16),
                  pltpu.SemaphoreType.DMA((2, 2)), pltpu.SemaphoreType.DMA((3, 2)))


def solution(mesh):
    def step(x, dy, gate, up, w_gate, w_up, w_down):
        comm = Comm(G, SPACING, CW)
        bf = jnp.bfloat16
        any_ = pl.BlockSpec(memory_space=pl.ANY)
        dma = pltpu.SemaphoreType.DMA
        return pl.pallas_call(
            lambda *refs: kernel(comm, *refs),
            name="mlp_backward",
            out_shape=[jax.ShapeDtypeStruct(s, bf) for s in ((T, D), (D, F), (D, F), (F, D))],
            in_specs=[any_] * 7,
            out_specs=[any_] * 4,
            scratch_shapes=comm.scratch() + [
                pltpu.VMEM((D, 2 * F), bf), pltpu.VMEM((D, 2 * F), bf), pltpu.VMEM((T, 2 * F), bf), pltpu.VMEM((R, 2 * F), bf),
                pltpu.VMEM((2 * F, T), bf), pltpu.VMEM((F, T), bf),
                dma((2,)), dma((2, PIECES)), dma((2, PIECES)), dma((NB // 2,)), dma((NB // 2,))],
            compiler_params=pltpu.CompilerParams(collective_id=0, has_side_effects=True, vmem_limit_bytes=67043328),
        )(x, dy, gate, up, w_gate, w_up, w_down)

    tokens, columns, rows = P("dp", None), P(None, "tp"), P("tp", None)
    return jax.shard_map(
        step,
        mesh=mesh,
        in_specs=(tokens, tokens, P("dp", "tp"), P("dp", "tp"), columns, columns, rows),
        out_specs=(tokens, P("dp", "tp"), P("dp", "tp"), P(("dp", "tp"), None)),
        check_vma=False,
    )
```

```python
import jax
import jax.numpy as jnp
from jax import lax
from jax.experimental import pallas as pl
from jax.experimental.pallas import tpu as pltpu
from jax.sharding import PartitionSpec as P

MESH = pl.DeviceIdType.MESH
R = 1024


class Comm:
    def __init__(self, G, D, cw, pA=320, KS=None):
        self.G, self.D, self.cw = G, D, cw
        self.K = KS or 3 * D
        self.a = pA; self.h = pA // 2; self.q = pA // 4
        self.e = R - 2 * pA; self.b = self.e // 4
        assert self.q % 16 == 0 and self.b % 16 == 0
        self.NS = 10
        self.rx = dict(A0=self.h, B0=self.h, A1=self.q, B1=self.q, A2=self.q, B2=self.q, A3=self.q, B3=self.q,
                       E0=3*self.b, E1=2*self.b, E2=self.b, EX=self.b, EY=self.b)
        off = 0; self.off = {}
        for k, v in self.rx.items():
            self.off[k] = off; off += v
        self.rxrows = off
        self.kinds = {}
        for i in range(8):
            self.kinds['A%d' % i] = len(self.kinds); self.kinds['B%d' % i] = len(self.kinds)
        for i in range(9):
            self.kinds['E%d' % i] = len(self.kinds)
        self.kinds['D'] = len(self.kinds)

    def scratch(self):
        n = len(self.kinds)
        return [pltpu.VMEM((self.K, self.rxrows, self.cw), jnp.bfloat16),
                pltpu.SemaphoreType.DMA((n, self.K)), pltpu.SemaphoreType.DMA((n, self.K)), pltpu.SemaphoreType.REGULAR]

    def bind(self, work, other, rxb, ssem, rsem, credit):
        self.work, self.other, self.rxb, self.ssem, self.rsem, self.credit = work, other, rxb, ssem, rsem, credit
        me = lax.axis_index("tp")
        core = me % 2; z = (me // 2) % 4; y = (me // 8) % 2; x = me // 16
        idx = lambda x, y, z, c: ((x * 2 + y) * 4 + z) * 2 + c
        self.core, self.z, self.y, self.x = core, z, y, x
        side = z // 2; self.side = side
        self.outer = jnp.logical_or(z == 0, z == 3); self.inner = jnp.logical_not(self.outer)
        zi = 1 + side
        zo = 3 * side
        self.px = idx(1 - x, y, z, core); self.py = idx(x, 1 - y, z, core)
        self.pc = idx(x, y, z, 1 - core)
        self.pin = idx(x, y, zi, core)
        self.pout = idx(x, y, zo, core)
        self.pacr = idx(x, y, 2 - side, core)
        m = lambda v: pl.multiple_of(v, 16)
        a, h, q, b = self.a, self.h, self.q, self.b
        e0 = 2 * a
        self.Ak = m(x * h); self.As = m((1 - x) * h)
        self.Aq = m(x * h + y * q); self.Aqs = m(x * h + (1 - y) * q)
        self.Bk = m(a + y * h); self.Bs = m(a + (1 - y) * h)
        self.Bq = m(a + y * h + x * q); self.Bqs = m(a + y * h + (1 - x) * q)
        self.Eex = m(e0 + (1 - side) * b); self.Efar = m(e0 + (1 - side) * 2 * b); self.Enear = m(e0 + side * 2 * b)
        self.Eown = m(e0 + z * b); self.Eout = m(e0 + zo * b)

    def barrier(self):
        bar = pltpu.get_barrier_semaphore()
        def sig(d): pl.semaphore_signal(bar, inc=1, device_id={"tp": d}, device_id_type=MESH)
        sig(self.px); sig(self.py); sig(self.pc)
        @pl.when(self.outer)
        def _(): sig(self.pin); pl.semaphore_wait(bar, 4)
        @pl.when(self.inner)
        def _(): sig(self.pout); sig(self.pacr); pl.semaphore_wait(bar, 5)

    def cp(self, kind, c, start, rows, dst_kind, dev):
        k = self.kinds[kind]; sl = c % self.K
        src = self.work.at[c, pl.ds(start, rows), :]
        if dst_kind is None: dst = src
        elif dst_kind == 'other': dst = self.other.at[c]
        else: dst = self.rxb.at[sl, pl.ds(self.off[dst_kind], rows), :]
        return pltpu.make_async_remote_copy(src_ref=src, dst_ref=dst, send_sem=self.ssem.at[k, sl], recv_sem=self.rsem.at[k, sl],
                                            device_id={"tp": dev}, device_id_type=MESH)

    def add(self, c, start, rows, rxk, roff=0):
        sl = c % self.K
        w = self.work.at[c, pl.ds(start, rows), :]
        v = w[...].astype(jnp.float32) + self.rxb[sl, pl.ds(self.off[rxk] + roff, rows), :].astype(jnp.float32)
        w[...] = v.astype(jnp.bfloat16)

    def stage(self, s, c):
        q, h, b = self.q, self.h, self.b
        C = self.cp
        A = [lambda: C('A0', c, self.As, h, 'A0', self.px), lambda: C('A1', c, self.Aqs, q, 'A1', self.py),
             lambda: C('A2', c, self.Aq, q, 'A2', self.pin), lambda: C('A3', c, self.Aq, q, 'A3', self.pacr),
             lambda: C('A4', c, self.Aq, q, None, self.pout), lambda: C('A5', c, self.Aq, q, None, self.py),
             lambda: C('A6', c, self.Ak, h, None, self.px)]
        B = [lambda: C('B0', c, self.Bs, h, 'B0', self.py), lambda: C('B1', c, self.Bqs, q, 'B1', self.px),
             lambda: C('B2', c, self.Bq, q, 'B2', self.pin), lambda: C('B3', c, self.Bq, q, 'B3', self.pacr),
             lambda: C('B4', c, self.Bq, q, None, self.pout), lambda: C('B5', c, self.Bq, q, None, self.px),
             lambda: C('B6', c, self.Bk, h, None, self.py)]
        E = [lambda: C('E0', c, self.Eex, 3*b, 'E0', self.pin), lambda: C('E1', c, self.Efar, 2*b, 'E1', self.pacr),
             lambda: C('E2', c, self.Eout, b, 'E2', self.pout), lambda: C('E3', c, self.Eown, b, 'EX', self.px),
             lambda: C('E4', c, self.Eown, b, 'EY', self.py), lambda: C('E5', c, self.Eown, b, None, self.pin),
             lambda: C('E6', c, self.Enear, 2*b, None, self.pacr), lambda: C('E7', c, self.Eex, 3*b, None, self.pout)]
        ws = lambda d: d().wait_send()
        wr = lambda d: d().wait_recv()
        st = lambda d: d().start()
        outer = lambda f: pl.when(self.outer)(f)
        inner = lambda f: pl.when(self.inner)(f)
        if s == 0:
            st(A[0]); st(B[0])
            @outer
            def _(): st(E[0])
        elif s == 1:
            @inner
            def _(): wr(E[0]); self.add(c, self.Eex, 3*b, 'E0'); st(E[1])
            @outer
            def _(): ws(E[0])
            A[0]().wait(); self.add(c, self.Ak, h, 'A0'); st(A[1])
            B[0]().wait(); self.add(c, self.Bk, h, 'B0'); st(B[1])
        elif s == 2:
            @inner
            def _(): E[1]().wait(); self.add(c, self.Enear, 2*b, 'E1'); st(E[2])
            A[1]().wait(); self.add(c, self.Aq, q, 'A1')
            @outer
            def _(): st(A[2])
            B[1]().wait(); self.add(c, self.Bq, q, 'B1')
            @outer
            def _(): st(B[2])
        elif s == 3:
            @inner
            def _():
                ws(E[2])
                wr(A[2]); self.add(c, self.Aq, q, 'A2'); st(A[3])
                wr(B[2]); self.add(c, self.Bq, q, 'B2'); st(B[3])
            @outer
            def _(): wr(E[2]); self.add(c, self.Eown, b, 'E2'); ws(A[2]); ws(B[2]); pl.semaphore_signal(self.credit, inc=1, device_id={"tp": self.pin}, device_id_type=MESH)
            st(E[3])
        elif s == 4:
            @inner
            def _():
                pl.semaphore_wait(self.credit, 1)
                A[3]().wait(); self.add(c, self.Aq, q, 'A3'); st(A[4])
                B[3]().wait(); self.add(c, self.Bq, q, 'B3'); st(B[4])
            E[3]().wait(); self.add(c, self.Eown, b, 'EX'); st(E[4])
        elif s == 5:
            E[4]().wait(); self.add(c, self.Eown, b, 'EY')
            @outer
            def _(): wr(A[4]); wr(B[4]); st(E[5])
            @inner
            def _(): ws(A[4])
            st(A[5])
            @inner
            def _(): ws(B[4])
            st(B[5])
        elif s == 6:
            @inner
            def _(): wr(E[5]); st(E[6])
            @outer
            def _(): ws(E[5])
            A[5]().wait(); st(A[6])
            B[5]().wait(); st(B[6])
        elif s == 7:
            @inner
            def _(): E[6]().wait(); st(E[7])
            A[6]().wait(); B[6]().wait()
        elif s == 8:
            @inner
            def _(): ws(E[7])
            @outer
            def _(): wr(E[7])
            st(lambda: C('D', c, 0, R, 'other', self.pc))
        elif s == 9:
            C('D', c, 0, R, 'other', self.pc).wait()

    def tick(self, t):
        for s in reversed(range(self.NS)):
            c = t - self.D * s
            @pl.when(jnp.logical_and(c >= 0, c < self.G))
            def _(s=s, c=c): self.stage(s, c)
    @property
    def nticks(self): return self.G + self.D * (self.NS - 1)


T, D, F = 2048, 5120, 384
G, SPACING, CW = 40, 2, 128
RB = 256
NB = T // RB
UW = 256
NU = D // UW
PIECES = 5
UNIT0 = 5


def nt(a, b):
    return lax.dot_general(a, b, (((1,), (1,)), ((), ())), preferred_element_type=jnp.float32)


def nn(a, b):
    return jnp.dot(a, b, preferred_element_type=jnp.float32)


def kernel(comm, x, dy, gate, up, w_gate, w_up, w_down, wown, wfar, work, other,
           rxb, ssem, rsem, credit, dall, dfar, dall_t, hid_t, own_sem, far_s, far_r, df_s, df_r):
    comm.bind(work, other, rxb, ssem, rsem, credit)
    mine = pl.multiple_of(comm.core * R, R)
    theirs = pl.multiple_of((1 - comm.core) * R, R)
    own = [pltpu.make_async_copy(w, wown.at[:, pl.ds(i * F, F)], own_sem.at[i]) for i, w in enumerate((w_gate, w_up))]
    PR = D // PIECES

    def far(i, p):
        rows = pl.ds(pl.multiple_of(p * PR, PR), PR)
        return pltpu.make_async_remote_copy(
            src_ref=(w_gate, w_up)[i].at[rows], dst_ref=wfar.at[rows, pl.ds(i * F, F)], send_sem=far_s.at[i, p],
            recv_sem=far_r.at[i, p], device_id={"tp": comm.pc}, device_id_type=MESH)

    def dsend(b):
        return pltpu.make_async_remote_copy(
            src_ref=dall.at[pl.ds(pl.multiple_of(theirs + b * RB, RB), RB)],
            dst_ref=dfar.at[pl.ds(pl.multiple_of(b * RB, RB), RB)], send_sem=df_s.at[b], recv_sem=df_r.at[b],
            device_id={"tp": comm.pc}, device_id_type=MESH)

    def hidden_part(wd, dyb, gb, ub, sem):
        wd_copy = pltpu.make_async_copy(w_down, wd, sem.at[3, 0])

        def row0(b):
            return pl.multiple_of(lax.rem(theirs + b * RB, T), RB)

        def load(b):
            rows, s = pl.ds(row0(b), RB), lax.rem(b, 2)
            return [pltpu.make_async_copy(a.at[rows], v.at[s], sem.at[i, s]) for i, (a, v) in enumerate(((dy, dyb), (gate, gb), (up, ub)))]

        wd_copy.start()
        for c in load(0):
            c.start()
        comm.barrier()
        for p in range(PIECES):
            for i in range(2):
                far(i, p).start()
        for c in own:
            c.start()
        wd_copy.wait()

        def step(b, _):
            @pl.when(b + 1 < NB)
            def _():
                for c in load(b + 1):
                    c.start()
            for c in load(b):
                c.wait()
            rows, s = pl.ds(row0(b), RB), lax.rem(b, 2)
            dh = nt(dyb[s], wd[...])
            g, u = gb[s].astype(jnp.float32), ub[s].astype(jnp.float32)
            sig = jax.nn.sigmoid(g)
            silu = g * sig
            d_up = (dh * silu).astype(jnp.bfloat16)
            d_gate = (dh * u * (sig + silu * (1.0 - sig))).astype(jnp.bfloat16)
            hid = (silu * u).astype(jnp.bfloat16)
            dall[rows, 0:F] = d_gate
            dall[rows, F:2 * F] = d_up
            dall_t[0:F, rows] = d_gate.T
            dall_t[F:2 * F, rows] = d_up.T
            hid_t[:, rows] = hid.T

            @pl.when(b < NB // 2)
            def _():
                dsend(b).start()
            return 0

        lax.fori_loop(0, NB, step, 0)

    pl.run_scoped(hidden_part, pltpu.VMEM((F, D), jnp.bfloat16), pltpu.VMEM((2, RB, D), jnp.bfloat16),
                  pltpu.VMEM((2, RB, F), jnp.bfloat16), pltpu.VMEM((2, RB, F), jnp.bfloat16), pltpu.SemaphoreType.DMA((4, 2)))

    def terms(pair):
        per = PR // (2 * CW)

        @pl.when(lax.rem(pair, per) == 0)
        def _():
            for i in range(2):
                far(i, pair // per).wait()
        rows = pl.ds(pl.multiple_of(pair * 2 * CW, 2 * CW), 2 * CW)
        for half in range(2):
            r = pl.ds(half * R // 2, R // 2)
            m = pl.ds(pl.multiple_of(mine + half * R // 2, R // 2), R // 2)
            t = nt(dall[m, :], wown[rows, :]) + nt(dfar[r, :], wfar[rows, :])
            t = t.astype(jnp.bfloat16)
            work[2 * pair, r, :] = t[:, :CW]
            work[2 * pair + 1, r, :] = t[:, CW:]

    def main_part(xb, dyb, lsem):
        def loads(u):
            s = lax.rem(u, 2)
            cols = pl.ds(pl.multiple_of(u * UW, UW), UW)
            return [pltpu.make_async_copy(x.at[:, cols], xb.at[s], lsem.at[0, s]),
                    pltpu.make_async_copy(dy.at[:, cols], dyb.at[s], lsem.at[1, s])]

        for c in loads(0):
            c.start()
        for b in range(NB // 2):
            dsend(b).wait()
        for c in own:
            c.wait()
        terms(0)

        def unit(u):
            s = lax.rem(u, 2)

            @pl.when(u + 1 < NU)
            def _():
                for c in loads(u + 1):
                    c.start()
            for c in loads(u):
                c.wait()

            rows = pl.ds(pl.multiple_of(u * UW, UW), UW)
            for i in range(2):
                wown[rows, pl.ds(i * F, F)] = nn(dall_t[pl.ds(i * F, F), :], xb[s]).T.astype(jnp.bfloat16)
            wfar[rows, 0:F] = nn(hid_t[...], dyb[s]).T.astype(jnp.bfloat16)

        def tick(t, _):
            comm.tick(t)
            pair = t // 2 + 1

            @pl.when(jnp.logical_and(lax.rem(t, 2) == 0, pair < G // 2))
            def _():
                terms(pair)
            u = (t - UNIT0) // 2

            @pl.when(jnp.logical_and(jnp.logical_and(t >= UNIT0, lax.rem(t - UNIT0, 2) == 0), u < NU))
            def _():
                unit(u)
            return 0

        lax.fori_loop(0, comm.nticks, tick, 0)

    pl.run_scoped(main_part, pltpu.VMEM((2, T, UW), jnp.bfloat16), pltpu.VMEM((2, T, UW), jnp.bfloat16), pltpu.SemaphoreType.DMA((2, 2)))


def write_out(dw, dwd_t, work, other, dx, dwg, dwu, dwd, stage, sem_x, sem_w, sem_d):
    copies = [pltpu.make_async_copy(dw.at[:, pl.ds(i * F, F)], o, sem_w.at[i]) for i, o in enumerate((dwg, dwu))]
    core = lax.rem(lax.axis_index("tp"), 2)
    for i, half in enumerate((work, other)):
        rows = pl.ds(pl.multiple_of(R * (core if i == 0 else 1 - core), R), R)
        copies += [pltpu.make_async_copy(half.at[c], dx.at[rows, pl.ds(c * CW, CW)], sem_x.at[i, c]) for c in range(G)]
    for c in copies:
        c.start()

    def put(u):
        s = lax.rem(u, 2)
        return pltpu.make_async_copy(stage.at[s], dwd.at[:, pl.ds(pl.multiple_of(u * UW, UW), UW)], sem_d.at[s])

    def flip(u, _):
        @pl.when(u >= 2)
        def _():
            put(u - 2).wait()
        stage[lax.rem(u, 2)] = dwd_t[pl.ds(pl.multiple_of(u * UW, UW), UW), 0:F].T
        put(u).start()
        return 0

    lax.fori_loop(0, NU, flip, 0)
    for c in copies + [put(NU - 2), put(NU - 1)]:
        c.wait()


def solution(mesh):
    def step(x, dy, gate, up, w_gate, w_up, w_down):
        comm = Comm(G, SPACING, CW)
        bf = jnp.bfloat16
        any_ = pl.BlockSpec(memory_space=pl.ANY)
        vmem = pl.BlockSpec(memory_space=pltpu.VMEM)
        dma = pltpu.SemaphoreType.DMA
        held = pl.pallas_call(
            lambda *refs: kernel(comm, *refs),
            name="mlp_backward",
            out_shape=[pltpu.VMEM(s, bf) for s in ((D, 2 * F), (D, 2 * F), (G, R, CW), (G, R, CW))],
            in_specs=[any_] * 7,
            out_specs=[vmem] * 4,
            scratch_shapes=comm.scratch() + [
                pltpu.VMEM((T, 2 * F), bf), pltpu.VMEM((R, 2 * F), bf), pltpu.VMEM((2 * F, T), bf), pltpu.VMEM((F, T), bf),
                dma((2,)), dma((2, PIECES)), dma((2, PIECES)), dma((NB // 2,)), dma((NB // 2,))],
            compiler_params=pltpu.CompilerParams(collective_id=0, has_side_effects=True, vmem_limit_bytes=26 * 2**20),
        )(x, dy, gate, up, w_gate, w_up, w_down)
        return pl.pallas_call(
            write_out,
            name="write_out",
            out_shape=[jax.ShapeDtypeStruct(s, bf) for s in ((T, D), (D, F), (D, F), (F, D))],
            in_specs=[vmem] * 4,
            out_specs=[any_] * 4,
            scratch_shapes=[pltpu.VMEM((2, F, UW), bf), dma((2, G)), dma((2,)), dma((2,))],
            compiler_params=pltpu.CompilerParams(vmem_limit_bytes=2**20),
        )(*held)

    tokens, columns, rows = P("dp", None), P(None, "tp"), P("tp", None)
    return jax.shard_map(
        step,
        mesh=mesh,
        in_specs=(tokens, tokens, P("dp", "tp"), P("dp", "tp"), columns, columns, rows),
        out_specs=(tokens, P("dp", "tp"), P("dp", "tp"), P(("dp", "tp"), None)),
        check_vma=False,
    )
```
